64 devices in a mesh: dp: 4 (over x, y), ep: 16 (over z, core).
Axes of the slice: x: 2, y: 2, z: 8, core: 2. Of those that a mesh axis runs over, the one named last changes fastest.
The devices are a block of a 4x4x8 slice.
Arguments:
- x: bfloat16 [4, 16, 256, 1792], P('dp', 'ep'), parts along dimension 0
- expert: int32 [4, 16, 256, 2], P('dp', 'ep'), parts along dimension 0
- slot: int32 [4, 16, 256, 2], P('dp', 'ep'), parts along dimension 0
- gate: float32 [4, 16, 256, 2], P('dp', 'ep'), parts along dimension 0
- w_gate: bfloat16 [32, 1792, 4864], P('ep')
- w_up: bfloat16 [32, 1792, 4864], P('ep')
- w_down: bfloat16 [32, 4864, 1792], P('ep')
Outputs:
- y: bfloat16 [4, 16, 256, 1792], P('dp', 'ep'), parts along dimension 0
There are 4 independent parts. The reference program is written for one: setup_inputs(seed, part) draws one part's arguments, and reference() takes and returns one part's arrays. A program takes and returns all parts, laid end to end along the dimension named above; an argument that names none is the same for every part.
All inputs are finite; a program needn't handle non-finite values.
Results may differ from the reference program's by a relative error of at most 0.009.
Values are sent between devices in bfloat16 or wider.
A program may use at most 768 MiB of HBM per device.

```python
import jax
import jax.numpy as jnp

MEMBERS = 16
TOKENS = 256
D = 1792
FF = 4864
TOP = 2
EXPERTS = 32
SLOTS = 5 * TOKENS * TOP // (4 * EXPERTS)


def setup_inputs(seed: int = 0, part: int = 0) -> dict:
    own, k1, k2, k3, k4, k5, k6 = jax.random.split(jax.random.key(seed), 7)
    kx, ke, kl, kg = jax.random.split(jax.random.fold_in(own, part), 4)
    devices = (1, MEMBERS)
    place = jax.random.permutation(kl, jnp.arange(EXPERTS, dtype=jnp.uint32))
    slow = ((EXPERTS + (9 * place) % EXPERTS) << ((9 * place) // EXPERTS)) // EXPERTS
    wait = (jax.random.bits(ke, (*devices, TOKENS, EXPERTS), jnp.uint32) >> 10) * slow
    expert = jnp.argsort(wait, axis=-1)[..., :TOP].astype(jnp.int32)
    chosen = jax.nn.one_hot(expert, EXPERTS, dtype=jnp.int32)
    in_line = jnp.cumsum(chosen.reshape(*devices, TOKENS * TOP, EXPERTS), axis=2) - 1
    slot = jnp.sum(in_line.reshape(chosen.shape) * chosen, axis=-1)

    def one(key, rows, columns):
        return (jax.random.normal(key, (rows, columns), jnp.float32) * rows**-0.5).astype(jnp.bfloat16)

    def weights(key, rows, columns):
        return jax.lax.map(lambda k: one(k, rows, columns), jax.random.split(key, EXPERTS))

    return {
        "x": jax.random.normal(kx, (*devices, TOKENS, D), jnp.float32).astype(jnp.bfloat16),
        "expert": expert,
        "slot": slot,
        "gate": jax.nn.softmax(jax.random.normal(kg, expert.shape, jnp.float32)),
        "w_gate": weights(k1, D, FF),
        "w_up": weights(k2, D, FF),
        "w_down": weights(k3, FF, D),
    }


def einsum(form, a, b):
    return jnp.einsum(form, a.astype(jnp.float32), b.astype(jnp.float32))


def reference(x, expert, slot, gate, w_gate, w_up, w_down):
    to_expert = jax.nn.one_hot(expert, EXPERTS, dtype=jnp.bfloat16)
    to_slot = jax.nn.one_hot(slot, SLOTS, dtype=jnp.bfloat16)
    weighted = to_expert * gate[..., None].astype(jnp.bfloat16)
    dispatch = einsum("abtke,abtkc->abtec", to_expert, to_slot).astype(jnp.bfloat16)
    combine = einsum("abtke,abtkc->abtec", weighted, to_slot).astype(jnp.bfloat16)
    z = einsum("abtec,abtd->aebcd", dispatch, x).astype(jnp.bfloat16)
    h = jax.nn.silu(einsum("aebcd,edf->aebcf", z, w_gate))
    h = (h * einsum("aebcd,edf->aebcf", z, w_up)).astype(jnp.bfloat16)
    out = einsum("aebcf,efd->aebcd", h, w_down).astype(jnp.bfloat16)
    y = einsum("abtec,aebcd->abtd", combine, out)
    return y.astype(jnp.bfloat16)
```

```python
import functools

import jax
import jax.numpy as jnp
from jax import lax
from jax.experimental import pallas as pl
from jax.experimental.pallas import tpu as pltpu
from jax.sharding import PartitionSpec as P

CORES = 2
TILE = 256
RING = 16
GROUP = 4
FAR = 1 << 16


def dot(a, b):
    return jnp.dot(a, b, preferred_element_type=jnp.float32)


def offsets(n):
    chips = n // CORES
    out = []
    for far in range(chips // 2, 0, -1):
        for way in (1, -1):
            if way == -1 and 2 * far == chips:
                continue
            for core in range(CORES):
                out.append(((way * far) % chips, core))
    return out + [(0, core) for core in range(CORES - 1, -1, -1)]


def kernel(n, slots, experts, flat_ref, gate_ref, x_hbm, wg_hbm, wu_hbm, wd_hbm, y_ref,
           xs, zsend, zrecv, osend, orecv, z, acc, yacc, hid, cols, gcols, wg, wu, wd,
           xsem, wsem, ssem, rsem):
    plan = offsets(n)
    self_at = n - 1
    chips = n // CORES
    me = lax.axis_index("ep")
    chip, core = me // CORES, lax.rem(me, CORES)
    dim = x_hbm.shape[1]
    half = dim // 2
    tokens = x_hbm.shape[0]
    rows = 2 * slots
    tiles = wd_hbm.shape[1] // TILE
    total = experts * tiles
    ring = wg.shape[0]

    def partner(i, back):
        ahead, other = plan[i]
        ahead = (chips - ahead) % chips if back else ahead
        return lax.rem(chip + ahead, chips) * CORES + lax.rem(core + other, CORES)

    def weight_copy(q, which):
        e, f = q // tiles, lax.rem(q, tiles)
        slot = lax.rem(q, ring)
        at = pl.ds(pl.multiple_of(f * TILE, TILE), TILE)
        if which == 2:
            return pltpu.make_async_copy(wd_hbm.at[e, at, :], wd.at[slot], wsem.at[2, slot])
        src, dst = ((wg_hbm, wg), (wu_hbm, wu))[which]
        return pltpu.make_async_copy(src.at[e, :, at], dst.at[slot], wsem.at[which, slot])

    def remote(phase, e, i, src, dst, back):
        return pltpu.make_async_remote_copy(
            src_ref=src.at[e, i], dst_ref=dst.at[e, i],
            send_sem=ssem.at[phase, i], recv_sem=rsem.at[phase, i],
            device_id={"ep": partner(i, back)}, device_id_type=pl.DeviceIdType.MESH)

    out_copy = lambda e, i: remote(e, e, i, zsend, zrecv, False)
    back_copy = lambda e, i: remote(experts + e, e, i, osend, orecv, True)

    xcopies = [pltpu.make_async_copy(x_hbm.at[:, pl.ds(k * half, half)], xs.at[pl.ds(k * tokens, tokens), :], xsem.at[k])
               for k in range(2)]
    for c in xcopies:
        c.start()

    barrier = pltpu.get_barrier_semaphore()
    for k in range(1, n):
        pl.semaphore_signal(barrier, inc=1, device_id={"ep": lax.rem(me + k, n)}, device_id_type=pl.DeviceIdType.MESH)

    @pl.loop(0, ring)
    def _(q):
        for which in range(3):
            weight_copy(q, which).start()

    def wanted(e, g, shape, axis):
        at = lax.broadcasted_iota(jnp.int32, shape, axis)
        want = jnp.zeros(shape, jnp.int32)
        for j in range(GROUP):
            inside = at - j * rows
            first = partner(g * GROUP + j, False) * (experts * slots) + e * slots
            value = first + inside + jnp.where(inside >= slots, FAR - slots, 0)
            want = jnp.where(inside >= 0, value, want)
        return want

    def dispatch(e, g):
        want = wanted(e, g, (GROUP * rows, 2 * tokens), 0)
        hit = (flat_ref[0:1, :] == want) | (flat_ref[1:2, :] == want)
        mask = jnp.where(hit, 1.0, 0.0).astype(jnp.bfloat16)
        packed = dot(mask, xs[...]).astype(jnp.bfloat16)
        for j in range(GROUP):
            i = g * GROUP + j
            piece = packed[j * rows:(j + 1) * rows]
            if i == self_at:
                zrecv[e, i] = piece
            else:
                zsend[e, i] = piece

    groups = n // GROUP
    for c in xcopies:
        c.wait()
    for g in range(groups):
        dispatch(0, g)
    pl.semaphore_wait(barrier, n - 1)
    for i in range(self_at):
        out_copy(0, i).start()
    for g in range(groups):
        dispatch(1, g)
    for k in range(2):
        cols[k] = jnp.broadcast_to(flat_ref[k:k + 1, :], (128, 2 * tokens)).T
        rounded = gate_ref[k:k + 1, :].astype(jnp.bfloat16).astype(jnp.float32)
        gcols[k] = jnp.broadcast_to(rounded, (128, 2 * tokens)).T
    for i in range(self_at):
        out_copy(0, i).wait_send()
        out_copy(1, i).start()

    quarter = GROUP * slots

    def spread(shape, axis, second):
        r = lax.broadcasted_iota(jnp.int32, shape, axis)
        step = jnp.zeros(shape, jnp.int32)
        for j in range(1, GROUP):
            step = step + jnp.where(r >= j * slots, slots, 0)
        return r + step + (slots if second else 0)

    def gather(e):
        shape = (quarter, GROUP * rows)
        there = lax.broadcasted_iota(jnp.int32, shape, 1)
        for g in range(groups):
            for j in range(GROUP):
                i = g * GROUP + j
                if i != self_at:
                    out_copy(e, i).wait_recv()
            got = zrecv[e, g * GROUP:(g + 1) * GROUP].reshape(GROUP * rows, half)
            for k in range(2):
                pick = jnp.where(there == spread(shape, 0, k == 1), 1.0, 0.0).astype(jnp.bfloat16)
                z[g * quarter:(g + 1) * quarter, k * half:(k + 1) * half] = dot(pick, got).astype(jnp.bfloat16)

    def up(q):
        slot = lax.rem(q, ring)
        weight_copy(q, 0).wait()
        weight_copy(q, 1).wait()
        a = dot(z[...], wg[slot])
        b = dot(z[...], wu[slot])
        return (jax.nn.silu(a) * b).astype(jnp.bfloat16)

    def refill(q, which):
        @pl.when(q + ring < total)
        def _():
            weight_copy(q + ring, which).start()

    def expert(e):
        base = e * tiles
        hid[0] = up(base)
        refill(base, 0)
        refill(base, 1)
        acc[...] = jnp.zeros_like(acc)

        def step(f, _):
            q = base + f
            weight_copy(q - 1, 2).wait()
            old = hid[lax.rem(f + 1, 2)]
            new = up(q)
            acc[...] += dot(old, wd[lax.rem(q - 1, ring)])
            hid[lax.rem(f, 2)] = new
            refill(q, 0)
            refill(q, 1)
            refill(q - 1, 2)
            return 0

        lax.fori_loop(1, tiles, step, 0)
        last = base + tiles - 1
        weight_copy(last, 2).wait()
        acc[...] += dot(hid[(tiles - 1) % 2], wd[last % ring])
        refill(last, 2)

    def give_back(e):
        shape = (GROUP * rows, quarter)
        there = lax.broadcasted_iota(jnp.int32, shape, 0)
        for g in range(groups):
            done = acc[g * quarter:(g + 1) * quarter, :].astype(jnp.bfloat16)
            packed = jnp.zeros((GROUP * rows, half), jnp.float32)
            for k in range(2):
                pick = jnp.where(there == spread(shape, 1, k == 1), 1.0, 0.0).astype(jnp.bfloat16)
                packed += dot(pick, done[:, k * half:(k + 1) * half])
            packed = packed.astype(jnp.bfloat16)
            for j in range(GROUP):
                i = g * GROUP + j
                piece = packed[j * rows:(j + 1) * rows]
                if i == self_at:
                    orecv[e, i] = piece
                else:
                    osend[e, i] = piece
            for j in range(GROUP):
                i = g * GROUP + j
                if i != self_at:
                    back_copy(e, i).start()

    def combine(e):
        shape = (2 * tokens, GROUP * rows)
        for g in range(groups):
            want = wanted(e, g, shape, 1)
            weight = jnp.zeros(shape, jnp.float32)
            for k in range(2):
                weight += jnp.where(cols[k, :, 0:1] == want, gcols[k, :, 0:1], 0.0)
            weight = weight.astype(jnp.bfloat16)
            for j in range(GROUP):
                i = g * GROUP + j
                if i != self_at:
                    back_copy(e, i).wait_recv()
            term = dot(weight, orecv[e, g * GROUP:(g + 1) * GROUP].reshape(GROUP * rows, half))
            if e == 0 and g == 0:
                yacc[...] = term
            else:
                yacc[...] += term

    for e in range(experts):
        gather(e)
        expert(e)
        give_back(e)
    for e in range(experts):
        combine(e)
    for k in range(2):
        y_ref[:, k * half:(k + 1) * half] = yacc[k * tokens:(k + 1) * tokens, :].astype(jnp.bfloat16)
    for i in range(self_at):
        out_copy(1, i).wait_send()
        for e in range(experts):
            back_copy(e, i).wait_send()


def solution(mesh):
    n = mesh.shape["ep"]

    def step(x, expert, slot, gate, w_gate, w_up, w_down):
        tokens, dim = x.shape[2:]
        top = expert.shape[3]
        experts, _, ff = w_gate.shape
        slots = 5 * tokens * top // (4 * experts * n)
        rows, half = 2 * slots, dim // 2
        expert, slot, gate = (v.reshape(tokens, top).T for v in (expert, slot, gate))
        flat = jnp.where(slot < slots, expert * slots + slot, -1)
        flat = jnp.concatenate([flat, flat + FAR], axis=1)
        gate = jnp.concatenate([gate, gate], axis=1)
        vmem = pl.BlockSpec(memory_space=pltpu.VMEM)
        hbm = pl.BlockSpec(memory_space=pl.ANY)
        bf16, f32 = jnp.bfloat16, jnp.float32
        message = lambda: pltpu.VMEM((experts, n, rows, half), bf16)
        y = pl.pallas_call(
            functools.partial(kernel, n, slots, experts),
            name="moe",
            out_shape=jax.ShapeDtypeStruct((tokens, dim), bf16),
            in_specs=[vmem, vmem] + [hbm] * 4,
            out_specs=vmem,
            scratch_shapes=[
                pltpu.VMEM((2 * tokens, half), bf16),
                message(), message(), message(), message(),
                pltpu.VMEM((n * slots, dim), bf16),
                pltpu.VMEM((n * slots, dim), f32),
                pltpu.VMEM((2 * tokens, half), f32),
                pltpu.VMEM((2, n * slots, TILE), bf16),
                pltpu.VMEM((top, 2 * tokens, 128), jnp.int32),
                pltpu.VMEM((top, 2 * tokens, 128), f32),
                pltpu.VMEM((RING, dim, TILE), bf16),
                pltpu.VMEM((RING, dim, TILE), bf16),
                pltpu.VMEM((RING, TILE, dim), bf16),
                pltpu.SemaphoreType.DMA((2,)),
                pltpu.SemaphoreType.DMA((3, RING)),
                pltpu.SemaphoreType.DMA((2 * experts, n - 1)),
                pltpu.SemaphoreType.DMA((2 * experts, n - 1)),
            ],
            compiler_params=pltpu.CompilerParams(
                collective_id=0, has_side_effects=True, vmem_limit_bytes=67_043_328),
        )(flat, gate, x.reshape(tokens, dim), w_gate, w_up, w_down)
        return y.reshape(x.shape)

    spread, held = P("dp", "ep"), P("ep")
    return jax.shard_map(
        step, mesh=mesh, in_specs=(spread,) * 4 + (held,) * 3, out_specs=spread, check_vma=False)
```

```python
import functools

import jax
import jax.numpy as jnp
from jax import lax
from jax.experimental import pallas as pl
from jax.experimental.pallas import tpu as pltpu
from jax.sharding import PartitionSpec as P

CORES = 2
TILE = 256
RING = 14
GROUP = 4
FAR = 1 << 16


def dot(a, b):
    return jnp.dot(a, b, preferred_element_type=jnp.float32)


def offsets(n):
    chips = n // CORES
    reach = range((chips - 1) // 2, 0, -1)
    out = [(ahead, core) for far in reach for core in range(CORES) for ahead in (far, chips - far)]
    out[2 * CORES:2 * CORES] = [(chips // 2, core) for core in range(CORES)]
    return out + [(0, core) for core in range(CORES - 1, -1, -1)]


def kernel(n, slots, experts, expert_hbm, slot_hbm, gate_hbm, x_hbm, wg_hbm, wu_hbm, wd_hbm, y_ref,
           eidx, sidx, gates, xs, zsend, zrecv, osend, orecv, z, acc, yacc, hid, cols, gcols, wg, wu, wd,
           xsem, wsem, ssem, rsem):
    plan = offsets(n)
    self_at = n - 1
    chips = n // CORES
    me = lax.axis_index("ep")
    chip, core = me // CORES, lax.rem(me, CORES)
    dim = x_hbm.shape[1]
    half = dim // 2
    tokens = x_hbm.shape[0]
    top = expert_hbm.shape[0]
    rows = 2 * slots
    tiles = wd_hbm.shape[1] // TILE
    total = experts * tiles
    ring = wg.shape[0]

    def partner(i, back):
        ahead, other = plan[i]
        ahead = (chips - ahead) % chips if back else ahead
        return lax.rem(chip + ahead, chips) * CORES + lax.rem(core + other, CORES)

    def weight_copy(q, which):
        e, f = q // tiles, lax.rem(q, tiles)
        slot = lax.rem(q, ring)
        at = pl.ds(pl.multiple_of(f * TILE, TILE), TILE)
        if which == 2:
            return pltpu.make_async_copy(wd_hbm.at[e, at, :], wd.at[slot], wsem.at[2, slot])
        src, dst = ((wg_hbm, wg), (wu_hbm, wu))[which]
        return pltpu.make_async_copy(src.at[e, :, at], dst.at[slot], wsem.at[which, slot])

    def remote(phase, e, i, src, dst, back):
        return pltpu.make_async_remote_copy(
            src_ref=src.at[e, i], dst_ref=dst.at[e, i],
            send_sem=ssem.at[phase, i], recv_sem=rsem.at[phase, i],
            device_id={"ep": partner(i, back)}, device_id_type=pl.DeviceIdType.MESH)

    out_copy = lambda e, i: remote(e, e, i, zsend, zrecv, False)
    back_copy = lambda e, i: remote(experts + e, e, i, osend, orecv, True)

    small = [pltpu.make_async_copy(src, dst, xsem.at[2 + k])
             for k, (src, dst) in enumerate(((expert_hbm, eidx), (slot_hbm, sidx), (gate_hbm, gates)))]
    halves = [pltpu.make_async_copy(x_hbm.at[:, pl.ds(k * half, half)], xs.at[pl.ds(k * tokens, tokens), :], xsem.at[k])
              for k in range(2)]
    for c in small + halves:
        c.start()

    barrier = pltpu.get_barrier_semaphore()
    for k in range(1, n):
        pl.semaphore_signal(barrier, inc=1, device_id={"ep": lax.rem(me + k, n)}, device_id_type=pl.DeviceIdType.MESH)

    for c in small:
        c.wait()
    line = jnp.where(sidx[...] < slots, eidx[...] * slots + sidx[...], -1)
    line = jnp.concatenate([line, line + FAR], axis=1)

    def wanted(e, g, shape, axis):
        at = lax.broadcasted_iota(jnp.int32, shape, axis)
        want = jnp.zeros(shape, jnp.int32)
        for j in range(GROUP):
            inside = at - j * rows
            first = partner(g * GROUP + j, False) * (experts * slots) + e * slots
            value = first + inside + jnp.where(inside >= slots, FAR - slots, 0)
            want = jnp.where(inside >= 0, value, want)
        return want

    def dispatch(e, g):
        want = wanted(e, g, (GROUP * rows, 2 * tokens), 0)
        hit = functools.reduce(jnp.logical_or, [line[k:k + 1, :] == want for k in range(top)])
        mask = jnp.where(hit, 1.0, 0.0).astype(jnp.bfloat16)
        packed = dot(mask, xs[...]).astype(jnp.bfloat16)
        for j in range(GROUP):
            i = g * GROUP + j
            piece = packed[j * rows:(j + 1) * rows]
            if i == self_at:
                zrecv[e, i] = piece
            else:
                zsend[e, i] = piece

    groups = n // GROUP
    for g in range(groups):
        if g == 0:
            for c in halves:
                c.wait()
        dispatch(0, g)
        if g == 0:
            pl.semaphore_wait(barrier, n - 1)
        for i in range(g * GROUP, min((g + 1) * GROUP, self_at)):
            out_copy(0, i).start()

    @pl.loop(0, ring)
    def _(q):
        for which in range(3):
            weight_copy(q, which).start()

    for g in range(groups):
        dispatch(1, g)
    rounded = gates[...].astype(jnp.bfloat16).astype(jnp.float32)
    rounded = jnp.concatenate([rounded, rounded], axis=1)
    for k in range(top):
        cols[k] = jnp.broadcast_to(line[k:k + 1, :], (128, 2 * tokens)).T
        gcols[k] = jnp.broadcast_to(rounded[k:k + 1, :], (128, 2 * tokens)).T
    for i in range(self_at):
        out_copy(0, i).wait_send()
        out_copy(1, i).start()

    quarter = GROUP * slots

    def spread(shape, axis, second):
        r = lax.broadcasted_iota(jnp.int32, shape, axis)
        step = jnp.zeros(shape, jnp.int32)
        for j in range(1, GROUP):
            step = step + jnp.where(r >= j * slots, slots, 0)
        return r + step + (slots if second else 0)

    def gather(e):
        shape = (quarter, GROUP * rows)
        there = lax.broadcasted_iota(jnp.int32, shape, 1)
        for g in range(groups):
            for j in range(GROUP):
                i = g * GROUP + j
                if i != self_at:
                    out_copy(e, i).wait_recv()
            got = zrecv[e, g * GROUP:(g + 1) * GROUP].reshape(GROUP * rows, half)
            for k in range(2):
                pick = jnp.where(there == spread(shape, 0, k == 1), 1.0, 0.0).astype(jnp.bfloat16)
                z[g * quarter:(g + 1) * quarter, k * half:(k + 1) * half] = dot(pick, got).astype(jnp.bfloat16)

    def up(q):
        slot = lax.rem(q, ring)
        weight_copy(q, 0).wait()
        weight_copy(q, 1).wait()
        a = dot(z[...], wg[slot])
        b = dot(z[...], wu[slot])
        return (jax.nn.silu(a) * b).astype(jnp.bfloat16)

    def refill(q, which):
        @pl.when(q + ring < total)
        def _():
            weight_copy(q + ring, which).start()

    def expert(e):
        base = e * tiles
        hid[0] = up(base)
        refill(base, 0)
        refill(base, 1)
        acc[...] = jnp.zeros_like(acc)

        def step(f, _):
            q = base + f
            weight_copy(q - 1, 2).wait()
            old = hid[lax.rem(f + 1, 2)]
            new = up(q)
            acc[...] += dot(old, wd[lax.rem(q - 1, ring)])
            hid[lax.rem(f, 2)] = new
            refill(q, 0)
            refill(q, 1)
            refill(q - 1, 2)
            return 0

        lax.fori_loop(1, tiles, step, 0)
        last = base + tiles - 1
        weight_copy(last, 2).wait()
        acc[...] += dot(hid[(tiles - 1) % 2], wd[last % ring])
        refill(last, 2)

    def give_back(e):
        shape = (GROUP * rows, quarter)
        there = lax.broadcasted_iota(jnp.int32, shape, 0)
        for g in range(groups):
            done = acc[g * quarter:(g + 1) * quarter, :].astype(jnp.bfloat16)
            packed = jnp.zeros((GROUP * rows, half), jnp.float32)
            for k in range(2):
                pick = jnp.where(there == spread(shape, 1, k == 1), 1.0, 0.0).astype(jnp.bfloat16)
                packed += dot(pick, done[:, k * half:(k + 1) * half])
            packed = packed.astype(jnp.bfloat16)
            for j in range(GROUP):
                i = g * GROUP + j
                piece = packed[j * rows:(j + 1) * rows]
                if i == self_at:
                    orecv[e, i] = piece
                else:
                    osend[e, i] = piece
            for j in range(GROUP):
                i = g * GROUP + j
                if i != self_at:
                    back_copy(e, i).start()

    def combine(e):
        shape = (2 * tokens, GROUP * rows)
        for g in range(groups):
            want = wanted(e, g, shape, 1)
            weight = jnp.zeros(shape, jnp.float32)
            for k in range(top):
                weight += jnp.where(cols[k, :, 0:1] == want, gcols[k, :, 0:1], 0.0)
            weight = weight.astype(jnp.bfloat16)
            for j in range(GROUP):
                i = g * GROUP + j
                if i != self_at:
                    back_copy(e, i).wait_recv()
            term = dot(weight, orecv[e, g * GROUP:(g + 1) * GROUP].reshape(GROUP * rows, half))
            if e == 0 and g == 0:
                yacc[...] = term
            elif e == experts - 1 and g == groups - 1:
                for k in range(2):
                    at = slice(k * tokens, (k + 1) * tokens)
                    y_ref[:, k * half:(k + 1) * half] = (yacc[at, :] + term[at]).astype(jnp.bfloat16)
            else:
                yacc[...] += term

    for e in range(experts):
        gather(e)
        expert(e)
        give_back(e)
    for e in range(experts):
        combine(e)
    for i in range(self_at):
        out_copy(1, i).wait_send()
        for e in range(experts):
            back_copy(e, i).wait_send()

def solution(mesh):
    n = mesh.shape["ep"]

    def step(x, expert, slot, gate, w_gate, w_up, w_down):
        tokens, dim = x.shape[2:]
        top = expert.shape[3]
        experts, _, ff = w_gate.shape
        slots = 5 * tokens * top // (4 * experts * n)
        rows, half = 2 * slots, dim // 2
        expert, slot, gate = (v.reshape(tokens, top).T for v in (expert, slot, gate))
        hbm = pl.BlockSpec(memory_space=pl.ANY)
        bf16, f32 = jnp.bfloat16, jnp.float32
        message = lambda: pltpu.VMEM((experts, n, rows, half), bf16)
        y = pl.pallas_call(
            functools.partial(kernel, n, slots, experts),
            name="moe",
            out_shape=pltpu.VMEM((tokens, dim), bf16),
            in_specs=[hbm] * 7,
            out_specs=pl.BlockSpec(memory_space=pltpu.VMEM),
            scratch_shapes=[
                pltpu.VMEM((top, tokens), jnp.int32),
                pltpu.VMEM((top, tokens), jnp.int32),
                pltpu.VMEM((top, tokens), f32),
                pltpu.VMEM((2 * tokens, half), bf16),
                message(), message(), message(), message(),
                pltpu.VMEM((n * slots, dim), bf16),
                pltpu.VMEM((n * slots, dim), f32),
                pltpu.VMEM((2 * tokens, half), f32),
                pltpu.VMEM((2, n * slots, TILE), bf16),
                pltpu.VMEM((top, 2 * tokens, 128), jnp.int32),
                pltpu.VMEM((top, 2 * tokens, 128), f32),
                pltpu.VMEM((RING, dim, TILE), bf16),
                pltpu.VMEM((RING, dim, TILE), bf16),
                pltpu.VMEM((RING, TILE, dim), bf16),
                pltpu.SemaphoreType.DMA((5,)),
                pltpu.SemaphoreType.DMA((3, RING)),
                pltpu.SemaphoreType.DMA((2 * experts, n - 1)),
                pltpu.SemaphoreType.DMA((2 * experts, n - 1)),
            ],
            compiler_params=pltpu.CompilerParams(
                collective_id=0, has_side_effects=True, vmem_limit_bytes=62_500_000),
        )(expert, slot, gate, x.reshape(tokens, dim), w_gate, w_up, w_down)
        return y.reshape(x.shape)

    spread, held = P("dp", "ep"), P("ep")
    return jax.shard_map(
        step, mesh=mesh, in_specs=(spread,) * 4 + (held,) * 3, out_specs=spread, check_vma=False)
```

```python
import functools

import jax
import jax.numpy as jnp
from jax import lax
from jax.experimental import pallas as pl
from jax.experimental.pallas import tpu as pltpu
from jax.sharding import PartitionSpec as P

CORES = 2
TILE = 256
RING = 14
GROUP = 4
FAR = 1 << 16


def dot(a, b):
    return jnp.dot(a, b, preferred_element_type=jnp.float32)


def offsets(n):
    chips = n // CORES
    both = lambda far: [(ahead, core) for core in range(CORES) for ahead in (far, chips - far)]
    reach = range((chips - 1) // 2, 1, -1)
    out = both(1) + [p for far in reach for p in both(far)]
    out[4 * CORES:4 * CORES] = [(chips // 2, core) for core in range(CORES)]
    return out + [(0, core) for core in range(CORES - 1, -1, -1)]


def near(n):
    chips = n // CORES
    step = (chips // 2 + 1) // 2
    return [(ahead % chips, core) for ahead in range(-step, step + 1) for core in range(CORES) if (ahead, core) != (0, 0)]


def kernel(n, slots, experts, expert_hbm, slot_hbm, gate_hbm, x_hbm, wg_hbm, wu_hbm, wd_hbm, y_ref,
           eidx, sidx, gates, xs, zsend, zrecv, osend, orecv, z, acc, yacc, hid, cols, gcols, wg, wu, wd,
           xsem, wsem, ssem, rsem, known):
    plan = offsets(n)
    self_at = n - 1
    chips = n // CORES
    me = lax.axis_index("ep")
    chip, core = me // CORES, lax.rem(me, CORES)
    dim = x_hbm.shape[1]
    half = dim // 2
    tokens = x_hbm.shape[0]
    top = expert_hbm.shape[0]
    rows = 2 * slots
    tiles = wd_hbm.shape[1] // TILE
    total = experts * tiles
    ring = wg.shape[0]

    def partner(i, back):
        ahead, other = plan[i]
        return device((chips - ahead) % chips if back else ahead, other)

    def greet(sem):
        for there in near(n):
            pl.semaphore_signal(sem, inc=1, device_id={"ep": device(*there)}, device_id_type=pl.DeviceIdType.MESH)

    def device(ahead, other):
        return lax.rem(chip + ahead, chips) * CORES + lax.rem(core + other, CORES)

    def weight_copy(q, which):
        e, f = q // tiles, lax.rem(q, tiles)
        slot = lax.rem(q, ring)
        at = pl.ds(pl.multiple_of(f * TILE, TILE), TILE)
        if which == 2:
            return pltpu.make_async_copy(wd_hbm.at[e, at, :], wd.at[slot], wsem.at[2, slot])
        src, dst = ((wg_hbm, wg), (wu_hbm, wu))[which]
        return pltpu.make_async_copy(src.at[e, :, at], dst.at[slot], wsem.at[which, slot])

    def remote(phase, e, i, src, dst, back):
        return pltpu.make_async_remote_copy(
            src_ref=src.at[e, i], dst_ref=dst.at[e, i],
            send_sem=ssem.at[phase, i], recv_sem=rsem.at[phase, i],
            device_id={"ep": partner(i, back)}, device_id_type=pl.DeviceIdType.MESH)

    out_copy = lambda e, i: remote(e, e, i, zsend, zrecv, False)
    back_copy = lambda e, i: remote(experts + e, e, i, osend, orecv, True)

    small = [pltpu.make_async_copy(src, dst, xsem.at[2 + k])
             for k, (src, dst) in enumerate(((expert_hbm, eidx), (slot_hbm, sidx), (gate_hbm, gates)))]
    halves = [pltpu.make_async_copy(x_hbm.at[:, pl.ds(k * half, half)], xs.at[pl.ds(k * tokens, tokens), :], xsem.at[k])
              for k in range(2)]
    for c in small + halves:
        c.start()

    barrier = pltpu.get_barrier_semaphore()
    greet(barrier)

    for c in small:
        c.wait()
    line = jnp.where(sidx[...] < slots, eidx[...] * slots + sidx[...], -1)
    line = jnp.concatenate([line, line + FAR], axis=1)

    def wanted(e, g, shape, axis):
        at = lax.broadcasted_iota(jnp.int32, shape, axis)
        want = jnp.zeros(shape, jnp.int32)
        for j in range(GROUP):
            inside = at - j * rows
            first = partner(g * GROUP + j, False) * (experts * slots) + e * slots
            value = first + inside + jnp.where(inside >= slots, FAR - slots, 0)
            want = jnp.where(inside >= 0, value, want)
        return want

    def dispatch(e, g):
        want = wanted(e, g, (GROUP * rows, 2 * tokens), 0)
        hit = functools.reduce(jnp.logical_or, [line[k:k + 1, :] == want for k in range(top)])
        mask = jnp.where(hit, 1.0, 0.0).astype(jnp.bfloat16)
        packed = dot(mask, xs[...]).astype(jnp.bfloat16)
        for j in range(GROUP):
            i = g * GROUP + j
            piece = packed[j * rows:(j + 1) * rows]
            if i == self_at:
                zrecv[e, i] = piece
            else:
                zsend[e, i] = piece

    groups = n // GROUP
    for g in range(groups):
        if g == 0:
            for c in halves:
                c.wait()
        dispatch(0, g)
        if g == 0:
            pl.semaphore_wait(barrier, len(near(n)))
            greet(known)
        if g == 1:
            pl.semaphore_wait(known, len(near(n)))
        for i in range(g * GROUP, min((g + 1) * GROUP, self_at)):
            out_copy(0, i).start()

    @pl.loop(0, ring)
    def _(q):
        for which in range(3):
            weight_copy(q, which).start()

    for g in range(groups):
        dispatch(1, g)
    rounded = gates[...].astype(jnp.bfloat16).astype(jnp.float32)
    rounded = jnp.concatenate([rounded, rounded], axis=1)
    for k in range(top):
        cols[k] = jnp.broadcast_to(line[k:k + 1, :], (128, 2 * tokens)).T
        gcols[k] = jnp.broadcast_to(rounded[k:k + 1, :], (128, 2 * tokens)).T
    for i in range(self_at):
        out_copy(0, i).wait_send()
        out_copy(1, i).start()

    quarter = GROUP * slots

    def spread(shape, axis, second):
        r = lax.broadcasted_iota(jnp.int32, shape, axis)
        step = jnp.zeros(shape, jnp.int32)
        for j in range(1, GROUP):
            step = step + jnp.where(r >= j * slots, slots, 0)
        return r + step + (slots if second else 0)

    def gather(e):
        shape = (quarter, GROUP * rows)
        there = lax.broadcasted_iota(jnp.int32, shape, 1)
        for g in range(groups):
            for j in range(GROUP):
                i = g * GROUP + j
                if i != self_at:
                    out_copy(e, i).wait_recv()
            got = zrecv[e, g * GROUP:(g + 1) * GROUP].reshape(GROUP * rows, half)
            for k in range(2):
                pick = jnp.where(there == spread(shape, 0, k == 1), 1.0, 0.0).astype(jnp.bfloat16)
                z[g * quarter:(g + 1) * quarter, k * half:(k + 1) * half] = dot(pick, got).astype(jnp.bfloat16)

    def up(q):
        slot = lax.rem(q, ring)
        weight_copy(q, 0).wait()
        weight_copy(q, 1).wait()
        a = dot(z[...], wg[slot])
        b = dot(z[...], wu[slot])
        return (jax.nn.silu(a) * b).astype(jnp.bfloat16)

    def refill(q, which):
        @pl.when(q + ring < total)
        def _():
            weight_copy(q + ring, which).start()

    def expert(e):
        base = e * tiles
        hid[0] = up(base)
        refill(base, 0)
        refill(base, 1)
        acc[...] = jnp.zeros_like(acc)

        def step(f, _):
            q = base + f
            weight_copy(q - 1, 2).wait()
            old = hid[lax.rem(f + 1, 2)]
            new = up(q)
            acc[...] += dot(old, wd[lax.rem(q - 1, ring)])
            hid[lax.rem(f, 2)] = new
            refill(q, 0)
            refill(q, 1)
            refill(q - 1, 2)
            return 0

        lax.fori_loop(1, tiles, step, 0)
        last = base + tiles - 1
        weight_copy(last, 2).wait()
        acc[...] += dot(hid[(tiles - 1) % 2], wd[last % ring])
        refill(last, 2)

    homeward = [*range(1, groups), 0]

    def give_back(e):
        shape = (GROUP * rows, quarter)
        there = lax.broadcasted_iota(jnp.int32, shape, 0)
        for g in homeward:
            done = acc[g * quarter:(g + 1) * quarter, :].astype(jnp.bfloat16)
            packed = jnp.zeros((GROUP * rows, half), jnp.float32)
            for k in range(2):
                pick = jnp.where(there == spread(shape, 1, k == 1), 1.0, 0.0).astype(jnp.bfloat16)
                packed += dot(pick, done[:, k * half:(k + 1) * half])
            packed = packed.astype(jnp.bfloat16)
            for j in range(GROUP):
                i = g * GROUP + j
                piece = packed[j * rows:(j + 1) * rows]
                if i == self_at:
                    orecv[e, i] = piece
                else:
                    osend[e, i] = piece
            for j in range(GROUP):
                i = g * GROUP + j
                if i != self_at:
                    back_copy(e, i).start()

    def combine(e):
        shape = (2 * tokens, GROUP * rows)
        for g in homeward:
            want = wanted(e, g, shape, 1)
            weight = jnp.zeros(shape, jnp.float32)
            for k in range(top):
                weight += jnp.where(cols[k, :, 0:1] == want, gcols[k, :, 0:1], 0.0)
            weight = weight.astype(jnp.bfloat16)
            for j in range(GROUP):
                i = g * GROUP + j
                if i != self_at:
                    back_copy(e, i).wait_recv()
            term = dot(weight, orecv[e, g * GROUP:(g + 1) * GROUP].reshape(GROUP * rows, half))
            if e == 0 and g == homeward[0]:
                yacc[...] = term
            elif e == experts - 1 and g == homeward[-1]:
                for k in range(2):
                    at = slice(k * tokens, (k + 1) * tokens)
                    y_ref[:, k * half:(k + 1) * half] = (yacc[at, :] + term[at]).astype(jnp.bfloat16)
            else:
                yacc[...] += term

    for e in range(experts):
        gather(e)
        expert(e)
        give_back(e)
    for e in range(experts):
        combine(e)
    for i in range(self_at):
        out_copy(1, i).wait_send()
        for e in range(experts):
            back_copy(e, i).wait_send()

def solution(mesh):
    n = mesh.shape["ep"]

    def step(x, expert, slot, gate, w_gate, w_up, w_down):
        tokens, dim = x.shape[2:]
        top = expert.shape[3]
        experts, _, ff = w_gate.shape
        slots = 5 * tokens * top // (4 * experts * n)
        rows, half = 2 * slots, dim // 2
        expert, slot, gate = (v.reshape(tokens, top).T for v in (expert, slot, gate))
        hbm = pl.BlockSpec(memory_space=pl.ANY)
        bf16, f32 = jnp.bfloat16, jnp.float32
        message = lambda: pltpu.VMEM((experts, n, rows, half), bf16)
        y = pl.pallas_call(
            functools.partial(kernel, n, slots, experts),
            name="moe",
            out_shape=pltpu.VMEM((tokens, dim), bf16),
            in_specs=[hbm] * 7,
            out_specs=pl.BlockSpec(memory_space=pltpu.VMEM),
            scratch_shapes=[
                pltpu.VMEM((top, tokens), jnp.int32),
                pltpu.VMEM((top, tokens), jnp.int32),
                pltpu.VMEM((top, tokens), f32),
                pltpu.VMEM((2 * tokens, half), bf16),
                message(), message(), message(), message(),
                pltpu.VMEM((n * slots, dim), bf16),
                pltpu.VMEM((n * slots, dim), f32),
                pltpu.VMEM((2 * tokens, half), f32),
                pltpu.VMEM((2, n * slots, TILE), bf16),
                pltpu.VMEM((top, 2 * tokens, 128), jnp.int32),
                pltpu.VMEM((top, 2 * tokens, 128), f32),
                pltpu.VMEM((RING, dim, TILE), bf16),
                pltpu.VMEM((RING, dim, TILE), bf16),
                pltpu.VMEM((RING, TILE, dim), bf16),
                pltpu.SemaphoreType.DMA((5,)),
                pltpu.SemaphoreType.DMA((3, RING)),
                pltpu.SemaphoreType.DMA((2 * experts, n - 1)),
                pltpu.SemaphoreType.DMA((2 * experts, n - 1)),
                pltpu.SemaphoreType.REGULAR,
            ],
            compiler_params=pltpu.CompilerParams(
                collective_id=0, has_side_effects=True, vmem_limit_bytes=62_500_000),
        )(expert, slot, gate, x.reshape(tokens, dim), w_gate, w_up, w_down)
        return y.reshape(x.shape)

    spread, held = P("dp", "ep"), P("ep")
    return jax.shard_map(
        step, mesh=mesh, in_specs=(spread,) * 4 + (held,) * 3, out_specs=spread, check_vma=False)
```

```python
import functools

import jax
import jax.numpy as jnp
from jax import lax
from jax.experimental import pallas as pl
from jax.experimental.pallas import tpu as pltpu
from jax.sharding import PartitionSpec as P

CORES = 2
TILE = 256
RING = 14
GROUP = 4
FAR = 1 << 16


def dot(a, b):
    return jnp.dot(a, b, preferred_element_type=jnp.float32)


def offsets(n):
    chips = n // CORES
    both = lambda far: [(ahead, core) for core in range(CORES) for ahead in (far, chips - far)]
    reach = range((chips - 1) // 2, 1, -1)
    out = both(1) + [p for far in reach for p in both(far)]
    out[4 * CORES:4 * CORES] = [(chips // 2, core) for core in range(CORES)]
    return out + [(0, core) for core in range(CORES - 1, -1, -1)]


def near(n):
    chips = n // CORES
    step = (chips // 2 + 1) // 2
    return [(ahead % chips, core) for ahead in range(-step, step + 1) for core in range(CORES) if (ahead, core) != (0, 0)]


def kernel(n, slots, experts, expert_hbm, slot_hbm, gate_hbm, x_hbm, wg_hbm, wu_hbm, wd_hbm, y_ref,
           eidx, sidx, gates, xs, zsend, zrecv, osend, orecv, z, acc, yacc, hid, cols, gcols, wg, wu, wd,
           xsem, wsem, ssem, rsem, known):
    plan = offsets(n)
    self_at = n - 1
    chips = n // CORES
    me = lax.axis_index("ep")
    chip, core = me // CORES, lax.rem(me, CORES)
    dim = x_hbm.shape[1]
    half = dim // 2
    tokens = x_hbm.shape[0]
    top = expert_hbm.shape[0]
    rows = 2 * slots
    tiles = wd_hbm.shape[1] // TILE
    total = experts * tiles
    ring = wg.shape[0]

    def partner(i, back):
        ahead, other = plan[i]
        return device((chips - ahead) % chips if back else ahead, other)

    def greet(sem):
        for there in near(n):
            pl.semaphore_signal(sem, inc=1, device_id={"ep": device(*there)}, device_id_type=pl.DeviceIdType.MESH)

    def device(ahead, other):
        return lax.rem(chip + ahead, chips) * CORES + lax.rem(core + other, CORES)

    def weight_copy(q, which):
        e, f = q // tiles, lax.rem(q, tiles)
        slot = lax.rem(q, ring)
        at = pl.ds(pl.multiple_of(f * TILE, TILE), TILE)
        if which == 2:
            return pltpu.make_async_copy(wd_hbm.at[e, at, :], wd.at[slot], wsem.at[2, slot])
        src, dst = ((wg_hbm, wg), (wu_hbm, wu))[which]
        return pltpu.make_async_copy(src.at[e, :, at], dst.at[slot], wsem.at[which, slot])

    def remote(phase, e, i, src, dst, back):
        return pltpu.make_async_remote_copy(
            src_ref=src.at[e, i], dst_ref=dst.at[e, i],
            send_sem=ssem.at[phase, i], recv_sem=rsem.at[phase, i],
            device_id={"ep": partner(i, back)}, device_id_type=pl.DeviceIdType.MESH)

    out_copy = lambda e, i: remote(e, e, i, zsend, zrecv, False)
    back_copy = lambda e, i: remote(experts + e, e, i, osend, orecv, True)

    small = [pltpu.make_async_copy(src, dst, xsem.at[2 + k])
             for k, (src, dst) in enumerate(((expert_hbm, eidx), (slot_hbm, sidx), (gate_hbm, gates)))]
    halves = [pltpu.make_async_copy(x_hbm.at[:, pl.ds(k * half, half)], xs.at[pl.ds(k * tokens, tokens), :], xsem.at[k])
              for k in range(2)]
    barrier = pltpu.get_barrier_semaphore()
    greet(barrier)
    for c in small + halves:
        c.start()

    for c in small:
        c.wait()
    line = jnp.where(sidx[...] < slots, eidx[...] * slots + sidx[...], -1)
    line = jnp.concatenate([line, line + FAR], axis=1)

    def wanted(e, g, shape, axis):
        at = lax.broadcasted_iota(jnp.int32, shape, axis)
        want = jnp.zeros(shape, jnp.int32)
        for j in range(GROUP):
            inside = at - j * rows
            first = partner(g * GROUP + j, False) * (experts * slots) + e * slots
            value = first + inside + jnp.where(inside >= slots, FAR - slots, 0)
            want = jnp.where(inside >= 0, value, want)
        return want

    def dispatch(e, g):
        want = wanted(e, g, (GROUP * rows, 2 * tokens), 0)
        hit = functools.reduce(jnp.logical_or, [line[k:k + 1, :] == want for k in range(top)])
        mask = jnp.where(hit, 1.0, 0.0).astype(jnp.bfloat16)
        packed = dot(mask, xs[...]).astype(jnp.bfloat16)
        for j in range(GROUP):
            i = g * GROUP + j
            piece = packed[j * rows:(j + 1) * rows]
            if i == self_at:
                zrecv[e, i] = piece
            else:
                zsend[e, i] = piece

    groups = n // GROUP
    for g in range(groups):
        if g == 0:
            for c in halves:
                c.wait()
        dispatch(0, g)
        if g == 0:
            pl.semaphore_wait(barrier, len(near(n)))
            greet(known)
        if g == 1:
            pl.semaphore_wait(known, len(near(n)))
        for i in range(g * GROUP, min((g + 1) * GROUP, self_at)):
            out_copy(0, i).start()

    @pl.loop(0, ring)
    def _(q):
        for which in range(3):
            weight_copy(q, which).start()

    for g in range(groups):
        dispatch(1, g)
    rounded = gates[...].astype(jnp.bfloat16).astype(jnp.float32)
    rounded = jnp.concatenate([rounded, rounded], axis=1)
    for k in range(top):
        cols[k] = jnp.broadcast_to(line[k:k + 1, :], (128, 2 * tokens)).T
        gcols[k] = jnp.broadcast_to(rounded[k:k + 1, :], (128, 2 * tokens)).T
    for i in range(self_at):
        out_copy(0, i).wait_send()
        out_copy(1, i).start()

    quarter = GROUP * slots

    def spread(shape, axis, second):
        r = lax.broadcasted_iota(jnp.int32, shape, axis)
        step = jnp.zeros(shape, jnp.int32)
        for j in range(1, GROUP):
            step = step + jnp.where(r >= j * slots, slots, 0)
        return r + step + (slots if second else 0)

    def gather(e):
        shape = (quarter, GROUP * rows)
        there = lax.broadcasted_iota(jnp.int32, shape, 1)
        for g in range(groups):
            for j in range(GROUP):
                i = g * GROUP + j
                if i != self_at:
                    out_copy(e, i).wait_recv()
            got = zrecv[e, g * GROUP:(g + 1) * GROUP].reshape(GROUP * rows, half)
            for k in range(2):
                pick = jnp.where(there == spread(shape, 0, k == 1), 1.0, 0.0).astype(jnp.bfloat16)
                z[g * quarter:(g + 1) * quarter, k * half:(k + 1) * half] = dot(pick, got).astype(jnp.bfloat16)

    def up(q):
        slot = lax.rem(q, ring)
        weight_copy(q, 0).wait()
        weight_copy(q, 1).wait()
        a = dot(z[...], wg[slot])
        b = dot(z[...], wu[slot])
        return (jax.nn.silu(a) * b).astype(jnp.bfloat16)

    def refill(q, which):
        @pl.when(q + ring < total)
        def _():
            weight_copy(q + ring, which).start()

    def expert(e):
        base = e * tiles
        hid[0] = up(base)
        refill(base, 0)
        refill(base, 1)
        acc[...] = jnp.zeros_like(acc)

        def step(f, _):
            q = base + f
            weight_copy(q - 1, 2).wait()
            old = hid[lax.rem(f + 1, 2)]
            new = up(q)
            acc[...] += dot(old, wd[lax.rem(q - 1, ring)])
            hid[lax.rem(f, 2)] = new
            refill(q, 0)
            refill(q, 1)
            refill(q - 1, 2)
            return 0

        lax.fori_loop(1, tiles, step, 0)
        last = base + tiles - 1
        weight_copy(last, 2).wait()
        acc[...] += dot(hid[(tiles - 1) % 2], wd[last % ring])
        refill(last, 2)

    homeward = [*range(1, groups), 0]

    def give_back(e):
        shape = (GROUP * rows, quarter)
        there = lax.broadcasted_iota(jnp.int32, shape, 0)
        for g in homeward:
            done = acc[g * quarter:(g + 1) * quarter, :].astype(jnp.bfloat16)
            packed = jnp.zeros((GROUP * rows, half), jnp.float32)
            for k in range(2):
                pick = jnp.where(there == spread(shape, 1, k == 1), 1.0, 0.0).astype(jnp.bfloat16)
                packed += dot(pick, done[:, k * half:(k + 1) * half])
            packed = packed.astype(jnp.bfloat16)
            for j in range(GROUP):
                i = g * GROUP + j
                piece = packed[j * rows:(j + 1) * rows]
                if i == self_at:
                    orecv[e, i] = piece
                else:
                    osend[e, i] = piece
            for j in range(GROUP):
                i = g * GROUP + j
                if i != self_at:
                    back_copy(e, i).start()

    def combine(e):
        shape = (2 * tokens, GROUP * rows)
        for g in homeward:
            want = wanted(e, g, shape, 1)
            weight = jnp.zeros(shape, jnp.float32)
            for k in range(top):
                weight += jnp.where(cols[k, :, 0:1] == want, gcols[k, :, 0:1], 0.0)
            weight = weight.astype(jnp.bfloat16)
            for j in range(GROUP):
                i = g * GROUP + j
                if i != self_at:
                    back_copy(e, i).wait_recv()
            term = dot(weight, orecv[e, g * GROUP:(g + 1) * GROUP].reshape(GROUP * rows, half))
            if e == 0 and g == homeward[0]:
                yacc[...] = term
            elif e == experts - 1 and g == homeward[-1]:
                for k in range(2):
                    at = slice(k * tokens, (k + 1) * tokens)
                    y_ref[:, k * half:(k + 1) * half] = (yacc[at, :] + term[at]).astype(jnp.bfloat16)
            else:
                yacc[...] += term

    for e in range(experts):
        gather(e)
        expert(e)
        give_back(e)
    for e in range(experts):
        combine(e)
    for i in range(self_at):
        out_copy(1, i).wait_send()
        for e in range(experts):
            back_copy(e, i).wait_send()

def solution(mesh):
    n = mesh.shape["ep"]

    def step(x, expert, slot, gate, w_gate, w_up, w_down):
        tokens, dim = x.shape[2:]
        top = expert.shape[3]
        experts, _, ff = w_gate.shape
        slots = 5 * tokens * top // (4 * experts * n)
        rows, half = 2 * slots, dim // 2
        expert, slot, gate = (v.reshape(tokens, top).T for v in (expert, slot, gate))
        hbm = pl.BlockSpec(memory_space=pl.ANY)
        bf16, f32 = jnp.bfloat16, jnp.float32
        message = lambda: pltpu.VMEM((experts, n, rows, half), bf16)
        y = pl.pallas_call(
            functools.partial(kernel, n, slots, experts),
            name="moe",
            out_shape=pltpu.VMEM((tokens, dim), bf16),
            in_specs=[hbm] * 7,
            out_specs=pl.BlockSpec(memory_space=pltpu.VMEM),
            scratch_shapes=[
                pltpu.VMEM((top, tokens), jnp.int32),
                pltpu.VMEM((top, tokens), jnp.int32),
                pltpu.VMEM((top, tokens), f32),
                pltpu.VMEM((2 * tokens, half), bf16),
                message(), message(), message(), message(),
                pltpu.VMEM((n * slots, dim), bf16),
                pltpu.VMEM((n * slots, dim), f32),
                pltpu.VMEM((2 * tokens, half), f32),
                pltpu.VMEM((2, n * slots, TILE), bf16),
                pltpu.VMEM((top, 2 * tokens, 128), jnp.int32),
                pltpu.VMEM((top, 2 * tokens, 128), f32),
                pltpu.VMEM((RING, dim, TILE), bf16),
                pltpu.VMEM((RING, dim, TILE), bf16),
                pltpu.VMEM((RING, TILE, dim), bf16),
                pltpu.SemaphoreType.DMA((5,)),
                pltpu.SemaphoreType.DMA((3, RING)),
                pltpu.SemaphoreType.DMA((2 * experts, n - 1)),
                pltpu.SemaphoreType.DMA((2 * experts, n - 1)),
                pltpu.SemaphoreType.REGULAR,
            ],
            compiler_params=pltpu.CompilerParams(
                collective_id=0, has_side_effects=True, vmem_limit_bytes=62_500_000),
        )(expert, slot, gate, x.reshape(tokens, dim), w_gate, w_up, w_down)
        return y.reshape(x.shape)

    spread, held = P("dp", "ep"), P("ep")
    return jax.shard_map(
        step, mesh=mesh, in_specs=(spread,) * 4 + (held,) * 3, out_specs=spread, check_vma=False)
```
